8 devices in a mesh: depth: 2 (over z, y), col: 2 (over x), row: 2 (over core).
Axes of the slice: x: 2, y: 2, z: 1, core: 2. Of those that a mesh axis runs over, the one named last changes fastest.
Arguments:
- a_mat: bfloat16 [4096, 4096], P(('row', 'depth'), 'col')
- b_mat: bfloat16 [4096, 4096], P(('row', 'depth'), 'col')
Outputs:
- output: bfloat16 [4096, 4096], P(('row', 'depth'), 'col')
All inputs are finite; a program needn't handle non-finite values.
Results may differ from the reference program's by a relative error of at most 0.001.
Values are sent between devices in bfloat16 or wider.
A program may use at most 1 GiB of HBM per device.

```python
import jax
import jax.numpy as jnp

N = 4096


def setup_inputs(seed: int = 0) -> dict:
    key_a, key_b = jax.random.split(jax.random.key(seed))
    unit_scale = N ** -0.25
    a_vals = jax.random.normal(key_a, (N, N), jnp.float32) + unit_scale
    b_vals = jax.random.normal(key_b, (N, N), jnp.float32) + unit_scale
    a_mat = (a_vals * unit_scale).astype(jnp.bfloat16)
    b_mat = (b_vals * unit_scale).astype(jnp.bfloat16)
    return {"a_mat": a_mat, "b_mat": b_mat}


def reference(a_mat, b_mat):
    return jnp.dot(a_mat, b_mat, preferred_element_type=jnp.float32).astype(jnp.bfloat16)
```

```python
import functools

import jax
import jax.numpy as jnp
from jax import lax
from jax.experimental import pallas as pl
from jax.experimental.pallas import tpu as pltpu
from jax.sharding import PartitionSpec as P

MESH = pl.DeviceIdType.MESH
BF16, F32 = jnp.bfloat16, jnp.float32

Q = 1024
ROWS, COLS = 1024, 2048

B_STEPS = [(0, 0, 256), (256, 256, 256), (512, 512, 256), (768, 768, 128), (960, 896, 64), (896, 960, 64)]
A_STEPS = [(3, 0, 512), (3, 512, 512), (2, 0, 512), (2, 512, 256), (2, 768, 128), (2, 896, 128)]
STEPS = len(B_STEPS)
LAST = STEPS - 1
TM, TN = 256, 512


def exchange_kernel(a_ref, b_ref, acc, alast, blast, a4, b4, apen, bpen,
                    la_sem, lb_sem, xs, xr, ys, yr, fs, ds, dr):
    dep, col, row = lax.axis_index("depth"), lax.axis_index("col"), lax.axis_index("row")
    x_nbr, y_nbr, sib = (dep, 1 - col, row), (1 - dep, col, row), (dep, col, 1 - row)
    pair = (row + col) % 2
    other = 1 - pair
    near = pl.multiple_of(dep * Q, Q)
    far = pl.multiple_of((1 - dep) * Q, Q)

    load_a = [
        pltpu.make_async_copy(a_ref.at[:, pl.ds(near, Q)], a4.at[0], la_sem.at[0]),
        pltpu.make_async_copy(a_ref.at[:, pl.ds(far, Q)], a4.at[1], la_sem.at[1]),
    ]
    load_b = pltpu.make_async_copy(b_ref, b4.at[2 * pair], lb_sem)

    barrier = pltpu.get_barrier_semaphore()
    for dev in (x_nbr, y_nbr, sib):
        pl.semaphore_signal(barrier, inc=1, device_id=dev, device_id_type=MESH)
    for copy in load_a:
        copy.start()
    load_b.start()
    pl.semaphore_wait(barrier, 3)

    def a_copy(step):
        slot, start, size = A_STEPS[step]
        src = a_ref.at[:, pl.ds(pl.multiple_of((near if slot == 2 else far) + start, 128), size)]
        dst = alast.at[:, pl.ds(0, 128)] if step == LAST else a4.at[slot, :, pl.ds(start, size)]
        return pltpu.make_async_remote_copy(src, dst, xs.at[step], xr.at[step], device_id=x_nbr, device_id_type=MESH)

    def b_place(step, which):
        s1, s3, size = B_STEPS[step]
        if step == LAST:
            return blast.at[pl.ds(pl.multiple_of(128 + which * 64, 64), size)]
        if step == LAST - 1:
            return bpen.at[pl.ds(pl.multiple_of((1 - which) * 64, 64), size)]
        return b4.at[2 * which + 1, pl.ds(s1, size)]

    def b_start(step, which):
        s1, s3, _ = B_STEPS[step]
        return pl.multiple_of(s1 + which * (s3 - s1), 64)

    def b_copy(step):
        size = B_STEPS[step][2]
        return pltpu.make_async_remote_copy(
            b_ref.at[pl.ds(b_start(step, pair), size)], b_place(step, pair), ys.at[step], yr.at[pair, step],
            device_id=y_nbr, device_id_type=MESH)

    def forward(step):
        return pltpu.make_async_remote_copy(
            b_place(step, pair), b_place(step, pair), fs.at[step], yr.at[pair, step],
            device_id=sib, device_id_type=MESH)

    def forwarded(step):
        return pltpu.make_async_remote_copy(
            b_place(step, other), b_place(step, other), fs.at[step], yr.at[other, step],
            device_id=sib, device_id_type=MESH)

    give = pltpu.make_async_remote_copy(b_ref, b4.at[2 * pair], ds, dr, device_id=sib, device_id_type=MESH)
    take = pltpu.make_async_remote_copy(b_ref, b4.at[2 * other], ds, dr, device_id=sib, device_id_type=MESH)

    for step in range(STEPS):
        a_copy(step).start()
        b_copy(step).start()
        if step == 0:
            give.start()

    def multiply(a_view, b_view, fresh=False):
        @pl.loop(0, (ROWS // TM) * (COLS // TN))
        def _(t):
            rows = pl.ds(pl.multiple_of((t // (COLS // TN)) * TM, TM), TM)
            cols = pl.ds(pl.multiple_of((t % (COLS // TN)) * TN, TN), TN)
            part = jnp.dot(a_view(rows), b_view(cols), preferred_element_type=F32)
            if fresh:
                acc[rows, cols] = part
            else:
                acc[rows, cols] += part

    def slot_product(slot, start, size, fresh=False):
        multiply(lambda r: a4[slot, r, pl.ds(start, size)], lambda c: b4[slot, pl.ds(start, size), c], fresh)

    for copy in load_a:
        copy.wait()
    load_b.wait()
    give.wait_send()
    take.wait_recv()
    slot_product(0, 0, Q, fresh=True)
    blast[pl.ds(0, 128), :] = b4[2, pl.ds(Q - 128, 128), :]

    for step in range(STEPS):
        b_copy(step).wait_recv()
        forward(step).start()
        a_copy(step).wait_recv()
        if step == 1:
            low = lax.broadcasted_iota(jnp.int32, (TM, 128), 1) < 64

            @pl.loop(0, ROWS // TM)
            def _(t):
                rows = pl.ds(pl.multiple_of(t * TM, TM), TM)
                a1, a3 = a4[1, rows, pl.ds(Q - 128, 128)], a4[3, rows, pl.ds(Q - 128, 128)]
                apen[rows, :] = jnp.where(low, a3, a1)
                alast[rows, pl.ds(128, 128)] = jnp.where(low, a1, a3)
        slot, start, size = A_STEPS[step]
        if slot == 2 and step != LAST:
            slot_product(2, start, size)
        forwarded(step).wait_recv()
        if step < LAST - 1:
            slot_product(1, B_STEPS[step][0], B_STEPS[step][2])
            slot_product(3, B_STEPS[step][1], B_STEPS[step][2])
        elif step == LAST - 1:
            multiply(lambda r: apen[r, :], lambda c: bpen[:, c])

    for step in range(STEPS):
        a_copy(step).wait_send()
        b_copy(step).wait_send()
        forward(step).wait_send()


def finish_kernel(acc, alast, blast, c_ref, stage, sem):
    blk = 128
    copies = []
    for t in range(ROWS // blk):
        rows = pl.ds(t * blk, blk)
        tail = jnp.dot(alast[rows, :], blast[...], preferred_element_type=F32)
        stage[rows, :] = (acc[rows, :] + tail).astype(BF16)
        copies.append(pltpu.make_async_copy(stage.at[rows], c_ref.at[rows], sem.at[t]))
        copies[-1].start()
    for copy in copies:
        copy.wait()


def solution(mesh):
    hbm = pl.BlockSpec(memory_space=pltpu.HBM)
    vmem = pl.BlockSpec(memory_space=pltpu.VMEM)
    dma = pltpu.SemaphoreType.DMA

    def local_product(a_blk, b_blk):
        a_blk = pltpu.with_memory_space_constraint(a_blk, pltpu.HBM)
        b_blk = pltpu.with_memory_space_constraint(b_blk, pltpu.HBM)
        acc, alast, blast = pl.pallas_call(
            exchange_kernel,
            out_shape=(
                pltpu.VMEM((ROWS, COLS), F32),
                pltpu.VMEM((ROWS, 256), BF16),
                pltpu.VMEM((256, COLS), BF16),
            ),
            in_specs=[hbm, hbm],
            out_specs=(vmem, vmem, vmem),
            scratch_shapes=[
                pltpu.VMEM((4, ROWS, Q), BF16),
                pltpu.VMEM((4, Q, COLS), BF16),
                pltpu.VMEM((ROWS, 128), BF16),
                pltpu.VMEM((128, COLS), BF16),
                dma((2,)), dma, dma((STEPS,)), dma((STEPS,)), dma((STEPS,)), dma((2, STEPS)), dma((STEPS,)), dma, dma,
            ],
            compiler_params=pltpu.CompilerParams(
                collective_id=0, has_side_effects=True, vmem_limit_bytes=44 * 2**20),
            name="exchange",
        )(a_blk, b_blk)
        return pl.pallas_call(
            finish_kernel,
            out_shape=pltpu.HBM((ROWS, COLS), BF16),
            in_specs=[vmem, vmem, vmem],
            out_specs=hbm,
            scratch_shapes=[pltpu.VMEM((ROWS, COLS), BF16), dma((8,))],
            compiler_params=pltpu.CompilerParams(vmem_limit_bytes=24 * 2**20),
            name="finish",
        )(acc, alast, blast)

    spec = P(("row", "depth"), "col")
    return jax.shard_map(local_product, mesh=mesh, in_specs=(spec, spec), out_specs=spec, check_vma=False)
```

```python
import functools

import jax
import jax.numpy as jnp
from jax import lax
from jax.experimental import pallas as pl
from jax.experimental.pallas import tpu as pltpu
from jax.sharding import PartitionSpec as P

MESH = pl.DeviceIdType.MESH
BF16, F32 = jnp.bfloat16, jnp.float32

Q = 1024
ROWS, COLS = 1024, 2048

B_STEPS = [(0, 0, 256), (256, 256, 256), (512, 512, 256), (768, 768, 128), (960, 896, 64), (896, 960, 64)]
A_STEPS = [(3, 0, 512), (3, 512, 512), (2, 0, 512), (2, 512, 256), (2, 768, 128), (2, 896, 128)]
STEPS = len(B_STEPS)
LAST = STEPS - 1
TM, TN = 512, 1024


def exchange_kernel(a_ref, b_ref, acc, alast, blast, a4, b4, apen, bpen,
                    ready, la_sem, lb_sem, xs, xr, ys, yr, fs, ds, dr):
    dep, col, row = lax.axis_index("depth"), lax.axis_index("col"), lax.axis_index("row")
    x_nbr, y_nbr, sib = (dep, 1 - col, row), (1 - dep, col, row), (dep, col, 1 - row)
    pair = (row + col) % 2
    other = 1 - pair
    near = pl.multiple_of(dep * Q, Q)
    far = pl.multiple_of((1 - dep) * Q, Q)

    load_a = [
        pltpu.make_async_copy(a_ref.at[:, pl.ds(near, Q)], a4.at[0], la_sem.at[0]),
        pltpu.make_async_copy(a_ref.at[:, pl.ds(far, Q)], a4.at[1], la_sem.at[1]),
    ]
    load_b = pltpu.make_async_copy(b_ref, b4.at[2 * pair], lb_sem)

    barrier = pltpu.get_barrier_semaphore()

    def tell(semaphore, dev):
        pl.semaphore_signal(semaphore, inc=1, device_id=dev, device_id_type=MESH)

    pl.when(col == 0)(lambda: tell(barrier, x_nbr))
    pl.when(dep == 0)(lambda: tell(barrier, y_nbr))
    pl.when(row == 1)(lambda: tell(barrier, sib))
    heard = col + dep + (1 - row)
    pl.when(heard > 0)(lambda: pl.semaphore_wait(barrier, heard))
    pl.when(col == 1)(lambda: tell(ready.at[0], x_nbr))
    pl.when(dep == 1)(lambda: tell(ready.at[1], y_nbr))
    pl.when(row == 0)(lambda: tell(ready.at[2], sib))

    def a_copy(step):
        slot, start, size = A_STEPS[step]
        src = a_ref.at[:, pl.ds(pl.multiple_of((near if slot == 2 else far) + start, 128), size)]
        dst = alast.at[:, pl.ds(0, 128)] if step == LAST else a4.at[slot, :, pl.ds(start, size)]
        return pltpu.make_async_remote_copy(src, dst, xs.at[step], xr.at[step], device_id=x_nbr, device_id_type=MESH)

    def b_place(step, which):
        s1, s3, size = B_STEPS[step]
        if step == LAST:
            return blast.at[pl.ds(pl.multiple_of(128 + which * 64, 64), size)]
        if step == LAST - 1:
            return bpen.at[pl.ds(pl.multiple_of((1 - which) * 64, 64), size)]
        return b4.at[2 * which + 1, pl.ds(s1, size)]

    def b_start(step, which):
        s1, s3, _ = B_STEPS[step]
        return pl.multiple_of(s1 + which * (s3 - s1), 64)

    def b_copy(step):
        size = B_STEPS[step][2]
        return pltpu.make_async_remote_copy(
            b_ref.at[pl.ds(b_start(step, pair), size)], b_place(step, pair), ys.at[step], yr.at[pair, step],
            device_id=y_nbr, device_id_type=MESH)

    def forward(step):
        return pltpu.make_async_remote_copy(
            b_place(step, pair), b_place(step, pair), fs.at[step], yr.at[pair, step],
            device_id=sib, device_id_type=MESH)

    def forwarded(step):
        return pltpu.make_async_remote_copy(
            b_place(step, other), b_place(step, other), fs.at[step], yr.at[other, step],
            device_id=sib, device_id_type=MESH)

    give = pltpu.make_async_remote_copy(b_ref, b4.at[2 * pair], ds, dr, device_id=sib, device_id_type=MESH)
    take = pltpu.make_async_remote_copy(b_ref, b4.at[2 * other], ds, dr, device_id=sib, device_id_type=MESH)

    def send_b():
        for step in range(STEPS):
            b_copy(step).start()

    pl.when(dep == 1)(send_b)
    pl.when(col == 0)(lambda: pl.semaphore_wait(ready.at[0], 1))
    for step in range(STEPS):
        a_copy(step).start()

    @pl.when(dep == 0)
    def _():
        pl.semaphore_wait(ready.at[1], 1)
        send_b()

    pl.when(row == 1)(lambda: pl.semaphore_wait(ready.at[2], 1))
    for copy in load_a:
        copy.start()
    load_b.start()
    give.start()

    def multiply(pairs, fresh=False):
        @pl.loop(0, (ROWS // TM) * (COLS // TN))
        def _(t):
            rows = pl.ds(pl.multiple_of((t // (COLS // TN)) * TM, TM), TM)
            cols = pl.ds(pl.multiple_of((t % (COLS // TN)) * TN, TN), TN)
            part = sum(jnp.dot(a_view(rows), b_view(cols), preferred_element_type=F32) for a_view, b_view in pairs)
            if fresh:
                acc[rows, cols] = part
            else:
                acc[rows, cols] += part

    def slot_pair(slot, start, size):
        return lambda r: a4[slot, r, pl.ds(start, size)], lambda c: b4[slot, pl.ds(start, size), c]

    for copy in load_a:
        copy.wait()
    load_b.wait()
    give.wait_send()
    take.wait_recv()
    multiply([slot_pair(0, 0, Q)], fresh=True)
    blast[pl.ds(0, 128), :] = b4[2, pl.ds(Q - 128, 128), :]

    for step in range(STEPS):
        b_copy(step).wait_recv()
        forward(step).start()
        a_copy(step).wait_recv()
        if step == 1:
            low = lax.broadcasted_iota(jnp.int32, (256, 128), 1) < 64

            @pl.loop(0, ROWS // 256)
            def _(t):
                rows = pl.ds(pl.multiple_of(t * 256, 256), 256)
                a1, a3 = a4[1, rows, pl.ds(Q - 128, 128)], a4[3, rows, pl.ds(Q - 128, 128)]
                apen[rows, :] = jnp.where(low, a3, a1)
                alast[rows, pl.ds(128, 128)] = jnp.where(low, a1, a3)
        slot, start, size = A_STEPS[step]
        forwarded(step).wait_recv()
        pairs = []
        if step < LAST - 1:
            pairs = [slot_pair(1, B_STEPS[step][0], B_STEPS[step][2]), slot_pair(3, B_STEPS[step][1], B_STEPS[step][2])]
        elif step == LAST - 1:
            pairs = [(lambda r: apen[r, :], lambda c: bpen[:, c])]
        if slot == 2 and step != LAST:
            pairs.append(slot_pair(2, start, size))
        if pairs:
            multiply(pairs)

    for step in range(STEPS):
        a_copy(step).wait_send()
        b_copy(step).wait_send()
        forward(step).wait_send()


def finish_kernel(acc, alast, blast, c_ref, stage, sem):
    blk = 128
    copies = []
    for t in range(ROWS // blk):
        rows = pl.ds(t * blk, blk)
        tail = jnp.dot(alast[rows, :], blast[...], preferred_element_type=F32)
        stage[rows, :] = (acc[rows, :] + tail).astype(BF16)
        copies.append(pltpu.make_async_copy(stage.at[rows], c_ref.at[rows], sem.at[t]))
        copies[-1].start()
    for copy in copies:
        copy.wait()


def solution(mesh):
    hbm = pl.BlockSpec(memory_space=pltpu.HBM)
    vmem = pl.BlockSpec(memory_space=pltpu.VMEM)
    dma = pltpu.SemaphoreType.DMA

    def local_product(a_blk, b_blk):
        a_blk = pltpu.with_memory_space_constraint(a_blk, pltpu.HBM)
        b_blk = pltpu.with_memory_space_constraint(b_blk, pltpu.HBM)
        acc, alast, blast = pl.pallas_call(
            exchange_kernel,
            out_shape=(
                pltpu.VMEM((ROWS, COLS), F32),
                pltpu.VMEM((ROWS, 256), BF16),
                pltpu.VMEM((256, COLS), BF16),
            ),
            in_specs=[hbm, hbm],
            out_specs=(vmem, vmem, vmem),
            scratch_shapes=[
                pltpu.VMEM((4, ROWS, Q), BF16),
                pltpu.VMEM((4, Q, COLS), BF16),
                pltpu.VMEM((ROWS, 128), BF16),
                pltpu.VMEM((128, COLS), BF16),
                pltpu.SemaphoreType.REGULAR((3,)),
                dma((2,)), dma, dma((STEPS,)), dma((STEPS,)), dma((STEPS,)), dma((2, STEPS)), dma((STEPS,)), dma, dma,
            ],
            compiler_params=pltpu.CompilerParams(
                collective_id=0, has_side_effects=True, vmem_limit_bytes=44 * 2**20),
            name="exchange",
        )(a_blk, b_blk)
        return pl.pallas_call(
            finish_kernel,
            out_shape=pltpu.HBM((ROWS, COLS), BF16),
            in_specs=[vmem, vmem, vmem],
            out_specs=hbm,
            scratch_shapes=[pltpu.VMEM((ROWS, COLS), BF16), dma((8,))],
            compiler_params=pltpu.CompilerParams(vmem_limit_bytes=24 * 2**20),
            name="finish",
        )(acc, alast, blast)

    spec = P(("row", "depth"), "col")
    return jax.shard_map(local_product, mesh=mesh, in_specs=(spec, spec), out_specs=spec, check_vma=False)
```

```python
import jax
import jax.numpy as jnp
from jax import lax
from jax.experimental import pallas as pl
from jax.experimental.pallas import tpu as pltpu
from jax.sharding import PartitionSpec as P

MESH = pl.DeviceIdType.MESH
BF16, F32 = jnp.bfloat16, jnp.float32

Q = 1024
ROWS, COLS = 1024, 2048

B_STEPS = [(0, 0, 512), (512, 512, 256), (768, 768, 128), (960, 896, 64), (896, 960, 64)]
A_STEPS = [(3, 0, 1024), (2, 0, 512), (2, 512, 256), (2, 768, 128), (2, 896, 128)]
LAST = len(B_STEPS) - 1
PEN = LAST - 1
EARLY = PEN
HALF = B_STEPS[LAST][2] // 2
TM, TN = 512, 1024


def exchange_kernel(a_ref, b_ref, acc, alast, blast, a4, b4, apen, bpen, relay_out, relay_in,
                    ready, loaded, sent, xr, yr, dr, rr):
    dep, col, row = lax.axis_index("depth"), lax.axis_index("col"), lax.axis_index("row")
    x_nbr, y_nbr, sib = (dep, 1 - col, row), (1 - dep, col, row), (dep, col, 1 - row)
    pair = (row + col) % 2
    other = 1 - pair
    near = pl.multiple_of(dep * Q, Q)
    far = pl.multiple_of((1 - dep) * Q, Q)
    main, more = sent.at[0], sent.at[1]

    def remote(src, dst, send_sem, recv_sem, dev):
        return pltpu.make_async_remote_copy(src, dst, send_sem, recv_sem, device_id=dev, device_id_type=MESH)

    barrier = pltpu.get_barrier_semaphore()

    def tell(semaphore, dev):
        pl.semaphore_signal(semaphore, inc=1, device_id=dev, device_id_type=MESH)

    pl.when(col == 0)(lambda: tell(barrier, x_nbr))
    pl.when(dep == 0)(lambda: tell(barrier, y_nbr))
    pl.when(row == 1)(lambda: tell(barrier, sib))
    heard = col + dep + (1 - row)
    pl.when(heard > 0)(lambda: pl.semaphore_wait(barrier, heard))
    pl.when(col == 1)(lambda: tell(ready.at[0], x_nbr))
    pl.when(dep == 1)(lambda: tell(ready.at[1], y_nbr))
    pl.when(row == 0)(lambda: tell(ready.at[2], sib))

    def a_copy(step, rows=ROWS):
        slot, start, size = A_STEPS[step]
        src = a_ref.at[pl.ds(0, rows), pl.ds(pl.multiple_of((near if slot == 2 else far) + start, 128), size)]
        dst = alast.at[pl.ds(0, rows), pl.ds(0, 128)] if step == LAST else a4.at[slot, :, pl.ds(start, size)]
        return remote(src, dst, main, xr.at[step], x_nbr)

    def b_start(step, which):
        s1, s3, _ = B_STEPS[step]
        return s1 + which * (s3 - s1)

    def b_place(step, which):
        if step == PEN:
            return bpen.at[pl.ds(pl.multiple_of((1 - which) * 64, 64), 64)]
        return b4.at[2 * which + 1, pl.ds(B_STEPS[step][0], B_STEPS[step][2])]

    def b_copy(step):
        src = b_ref.at[pl.ds(pl.multiple_of(b_start(step, pair), 64), B_STEPS[step][2])]
        return remote(src, b_place(step, pair), main, yr.at[pair, step], y_nbr)

    def forward(step, which):
        return remote(b_place(step, which), b_place(step, which), main, yr.at[which, step], sib)

    def tail_place(which, half):
        return blast.at[pl.ds(pl.multiple_of(128 + which * 64 + half * HALF, HALF), HALF)]

    def tail_copy(half):
        src = b_ref.at[pl.ds(pl.multiple_of(b_start(LAST, pair) + half * HALF, HALF), HALF)]
        return remote(src, tail_place(pair, half), main, yr.at[pair, LAST + half], y_nbr)

    def tail_forward(which, half, sem=main):
        return remote(tail_place(which, half), tail_place(which, half), sem, yr.at[which, LAST + half], sib)

    extra = remote(
        b4.at[2 * other, pl.ds(pl.multiple_of(b_start(LAST, other) + HALF, HALF), HALF)], tail_place(other, 1),
        more, yr.at[other, LAST + 1], y_nbr)
    relay_rows = pl.ds(ROWS // 2, ROWS // 2)
    relay_cols = pl.ds(pl.multiple_of(near + A_STEPS[LAST][1], 128), 128)
    relay_give = remote(a_ref.at[relay_rows, relay_cols], relay_out, main, rr.at[0], sib)
    relay_send = remote(relay_out, relay_in, more, rr.at[1], x_nbr)
    relay_end = remote(relay_in, alast.at[relay_rows, pl.ds(0, 128)], more, rr.at[0], sib)

    give = remote(b_ref, b4.at[2 * pair], main, dr, sib)
    take = remote(b_ref, b4.at[2 * other], main, dr, sib)

    def send_b():
        for step in range(EARLY):
            b_copy(step).start()

    pl.when(dep == 1)(send_b)
    pl.when(col == 0)(lambda: pl.semaphore_wait(ready.at[0], 1))
    for step in range(EARLY):
        a_copy(step).start()

    @pl.when(dep == 0)
    def _():
        pl.semaphore_wait(ready.at[1], 1)
        send_b()

    pl.when(row == 1)(lambda: pl.semaphore_wait(ready.at[2], 1))
    pltpu.make_async_copy(a_ref.at[:, pl.ds(near, Q)], a4.at[0], loaded).start()
    pltpu.make_async_copy(a_ref.at[:, pl.ds(far, Q)], a4.at[1], loaded).start()
    pltpu.make_async_copy(b_ref, b4.at[2 * pair], loaded).start()

    @pl.when(row == 0)
    def _():
        relay_give.start()
        a_copy(PEN).start()
        b_copy(PEN).start()
        a_copy(LAST, ROWS // 2).start()
        tail_copy(0).start()

    give.start()

    @pl.when(row == 1)
    def _():
        relay_give.wait_recv()
        relay_send.start()
        a_copy(PEN).start()
        a_copy(LAST).start()

    pltpu.make_async_copy(b4.at[pl.ds(0, 2)], b4.at[pl.ds(0, 2)], loaded).wait()
    take.wait_recv()

    @pl.when(row == 1)
    def _():
        extra.start()
        b_copy(PEN).start()
        tail_copy(0).start()
        tail_copy(1).start()

    def multiply(a_view, b_view, fresh=False):
        @pl.loop(0, (ROWS // TM) * (COLS // TN))
        def _(t):
            rows = pl.ds(pl.multiple_of((t // (COLS // TN)) * TM, TM), TM)
            cols = pl.ds(pl.multiple_of((t % (COLS // TN)) * TN, TN), TN)
            part = jnp.dot(a_view(rows), b_view(cols), preferred_element_type=F32)
            if fresh:
                acc[rows, cols] = part
            else:
                acc[rows, cols] += part

    multiply(lambda r: a4[0, r, :], lambda c: b4[0, :, c], fresh=True)
    blast[pl.ds(0, 128), :] = b4[2, pl.ds(Q - 128, 128), :]

    for step in range(PEN):
        b_copy(step).wait_recv()
        forward(step, pair).start()
        a_copy(step).wait_recv()
        if step == 0:
            low = lax.broadcasted_iota(jnp.int32, (256, 128), 1) < 64

            @pl.loop(0, ROWS // 256)
            def _(t):
                rows = pl.ds(pl.multiple_of(t * 256, 256), 256)
                a1, a3 = a4[1, rows, pl.ds(Q - 128, 128)], a4[3, rows, pl.ds(Q - 128, 128)]
                apen[rows, :] = jnp.where(low, a3, a1)
                alast[rows, pl.ds(128, 128)] = jnp.where(low, a1, a3)

        forward(step, other).wait_recv()
        parts = [(slot, pl.ds(B_STEPS[step][0], B_STEPS[step][2])) for slot in (1, 3)]
        slot, start, size = A_STEPS[step]
        if slot == 2:
            parts.append((2, pl.ds(start, size)))
        multiply(lambda r: jnp.concatenate([a4[s, r, k] for s, k in parts], axis=1),
                 lambda c: jnp.concatenate([b4[s, k, c] for s, k in parts], axis=0))

    @pl.when(row == 1)
    def _():
        relay_send.wait_recv()
        relay_end.start()
        extra.wait_recv()
        tail_forward(other, 1, more).start()

    b_copy(PEN).wait_recv()
    forward(PEN, pair).start()
    a_copy(PEN).wait_recv()

    @pl.when(row == 0)
    def _():
        tail_copy(0).wait_recv()
        tail_forward(pair, 0).start()

    forward(PEN, other).wait_recv()
    pen_cols = pl.ds(A_STEPS[PEN][1], 128)
    multiply(lambda r: jnp.concatenate([apen[r, :], a4[2, r, pen_cols]], axis=1),
             lambda c: jnp.concatenate([bpen[:, c], b4[2, pen_cols, c]], axis=0))

    @pl.when(row == 0)
    def _():
        a_copy(LAST, ROWS // 2).wait_recv()
        relay_end.wait_recv()
        tail_forward(pair, 1).wait_recv()
        tail_forward(other, 0).wait_recv()
        tail_forward(other, 1).wait_recv()
        every = b4.at[:, pl.ds(0, Q - Q // 64)]
        pltpu.make_async_copy(every, every, main).wait()

    @pl.when(row == 1)
    def _():
        for half in range(2):
            tail_copy(half).wait_recv()
            tail_forward(pair, half).start()
        a_copy(LAST).wait_recv()
        tail_forward(other, 0).wait_recv()
        pltpu.make_async_copy(b4, b4, main).wait()
        pltpu.make_async_copy(bpen, bpen, more).wait()


def finish_kernel(acc, alast, blast, c_ref, stage, done):
    blk = 128
    for t in range(ROWS // blk):
        rows = pl.ds(t * blk, blk)
        tail = jnp.dot(alast[rows, :], blast[...], preferred_element_type=F32)
        stage[rows, :] = (acc[rows, :] + tail).astype(BF16)
        pltpu.make_async_copy(stage.at[rows], c_ref.at[rows], done).start()
    pltpu.make_async_copy(stage, c_ref, done).wait()


def solution(mesh):
    hbm = pl.BlockSpec(memory_space=pltpu.HBM)
    vmem = pl.BlockSpec(memory_space=pltpu.VMEM)
    dma = pltpu.SemaphoreType.DMA

    def local_product(a_blk, b_blk):
        a_blk = pltpu.with_memory_space_constraint(a_blk, pltpu.HBM)
        b_blk = pltpu.with_memory_space_constraint(b_blk, pltpu.HBM)
        acc, alast, blast = pl.pallas_call(
            exchange_kernel,
            out_shape=(
                pltpu.VMEM((ROWS, COLS), F32),
                pltpu.VMEM((ROWS, 256), BF16),
                pltpu.VMEM((256, COLS), BF16),
            ),
            in_specs=[hbm, hbm],
            out_specs=(vmem, vmem, vmem),
            scratch_shapes=[
                pltpu.VMEM((4, ROWS, Q), BF16),
                pltpu.VMEM((4, Q, COLS), BF16),
                pltpu.VMEM((ROWS, 128), BF16),
                pltpu.VMEM((128, COLS), BF16),
                pltpu.VMEM((ROWS // 2, 128), BF16),
                pltpu.VMEM((ROWS // 2, 128), BF16),
                pltpu.SemaphoreType.REGULAR((3,)),
                dma, dma((2,)), dma((LAST + 1,)), dma((2, LAST + 2)), dma, dma((2,)),
            ],
            compiler_params=pltpu.CompilerParams(
                collective_id=0, has_side_effects=True, vmem_limit_bytes=44 * 2**20),
            name="exchange",
        )(a_blk, b_blk)
        return pl.pallas_call(
            finish_kernel,
            out_shape=pltpu.HBM((ROWS, COLS), BF16),
            in_specs=[vmem, vmem, vmem],
            out_specs=hbm,
            scratch_shapes=[pltpu.VMEM((ROWS, COLS), BF16), dma],
            compiler_params=pltpu.CompilerParams(vmem_limit_bytes=24 * 2**20),
            name="finish",
        )(acc, alast, blast)

    spec = P(("row", "depth"), "col")
    return jax.shard_map(local_product, mesh=mesh, in_specs=(spec, spec), out_specs=spec, check_vma=False)
```

```python
import jax
import jax.numpy as jnp
from jax import lax
from jax.experimental import pallas as pl
from jax.experimental.pallas import tpu as pltpu
from jax.sharding import PartitionSpec as P

MESH = pl.DeviceIdType.MESH
BF16, F32 = jnp.bfloat16, jnp.float32

Q = 1024
ROWS, COLS = 1024, 2048

B_STEPS = [(0, 512, 0, COLS), (512, 256, 0, COLS), (768, 128, 0, COLS), (896, 128, 0, 1024), (896, 128, 1024, 768),
           (896, 128, 1792, 256)]
A_STEPS = [(3, 0, ROWS), (2, 0, 512), (2, 512, 256), (2, 768, 128), (2, 896, 128)]
EARLY = 3
PEN, TAIL, END = 3, 4, 5
LAST = 4
LEFT = 1024
KEEP = 64
TN = 1024


def exchange_kernel(a_ref, b_ref, acc, left, alast, blast, a4, b4, relay_out, relay_in,
                    ready, loaded, sent, xr, yr, dr, rr):
    dep, col, row = lax.axis_index("depth"), lax.axis_index("col"), lax.axis_index("row")
    x_nbr, y_nbr, sib = (dep, 1 - col, row), (1 - dep, col, row), (dep, col, 1 - row)
    pair = (row + col) % 2
    other = 1 - pair
    near = pl.multiple_of(dep * Q, Q)
    far = pl.multiple_of((1 - dep) * Q, Q)
    main, more = sent.at[0], sent.at[1]

    def remote(src, dst, send_sem, recv_sem, dev):
        return pltpu.make_async_remote_copy(src, dst, send_sem, recv_sem, device_id=dev, device_id_type=MESH)

    barrier = pltpu.get_barrier_semaphore()

    def tell(semaphore, dev):
        pl.semaphore_signal(semaphore, inc=1, device_id=dev, device_id_type=MESH)

    pl.when(col == 0)(lambda: tell(barrier, x_nbr))
    pl.when(dep == 0)(lambda: tell(barrier, y_nbr))
    pl.when(row == 1)(lambda: tell(barrier, sib))
    heard = col + dep + (1 - row)
    pl.when(heard > 0)(lambda: pl.semaphore_wait(barrier, heard))
    pl.when(col == 1)(lambda: tell(ready.at[0], x_nbr))
    pl.when(dep == 1)(lambda: tell(ready.at[1], y_nbr))
    pl.when(row == 0)(lambda: tell(ready.at[2], sib))

    def a_copy(step, keep=None):
        slot, first, rows = A_STEPS[step]
        rows = pl.ds(first, keep or rows)
        src = a_ref.at[rows, pl.ds(near if slot == 2 else far, Q)]
        return remote(src, a4.at[slot, rows], main, xr.at[step], x_nbr)

    def b_place(step, which):
        r, rows, c, cols = B_STEPS[step]
        if step >= TAIL:
            return blast.at[pl.ds(pl.multiple_of(which * rows, rows), rows), pl.ds(c - LEFT, cols)]
        return b4.at[2 * which + 1, pl.ds(r, rows), pl.ds(c, cols)]

    def b_copy(step):
        r, rows, c, cols = B_STEPS[step]
        return remote(b_ref.at[pl.ds(r, rows), pl.ds(c, cols)], b_place(step, pair), main, yr.at[pair, step], y_nbr)

    def forward(step, which, sem=main):
        return remote(b_place(step, which), b_place(step, which), sem, yr.at[which, step], sib)

    end_rows, end_cols = pl.ds(B_STEPS[END][0], B_STEPS[END][1]), pl.ds(B_STEPS[END][2], B_STEPS[END][3])
    extra = remote(b4.at[2 * other, end_rows, end_cols], b_place(END, other), more, yr.at[other, END], y_nbr)
    relay_rows = pl.ds(A_STEPS[LAST][1] + KEEP, A_STEPS[LAST][2] - KEEP)
    relay_give = remote(a_ref.at[relay_rows, pl.ds(near, Q)], relay_out, more, rr.at[0], sib)
    relay_send = remote(relay_out, relay_in, more, rr.at[1], x_nbr)
    relay_end = remote(relay_in, a4.at[2, relay_rows], more, rr.at[0], sib)

    give = remote(b_ref, b4.at[2 * pair], main, dr, sib)
    take = remote(b_ref, b4.at[2 * other], main, dr, sib)

    def send_b():
        for step in range(EARLY):
            b_copy(step).start()

    pl.when(dep == 1)(send_b)
    pl.when(col == 0)(lambda: pl.semaphore_wait(ready.at[0], 1))
    for step in range(EARLY):
        a_copy(step).start()

    @pl.when(dep == 0)
    def _():
        pl.semaphore_wait(ready.at[1], 1)
        send_b()

    pl.when(row == 1)(lambda: pl.semaphore_wait(ready.at[2], 1))
    pltpu.make_async_copy(a_ref.at[:, pl.ds(near, Q)], a4.at[0], loaded).start()
    pltpu.make_async_copy(a_ref.at[:, pl.ds(far, Q)], a4.at[1], loaded).start()
    pltpu.make_async_copy(b_ref, b4.at[2 * pair], loaded).start()

    @pl.when(row == 0)
    def _():
        relay_give.start()
        a_copy(PEN).start()
        a_copy(LAST, KEEP).start()
        b_copy(PEN).start()
        b_copy(TAIL).start()

    give.start()

    @pl.when(row == 1)
    def _():
        relay_give.wait_recv()
        relay_send.start()
        a_copy(PEN).start()
        a_copy(LAST).start()

    pltpu.make_async_copy(b4.at[pl.ds(0, 2)], b4.at[pl.ds(0, 2)], loaded).wait()
    take.wait_recv()

    @pl.when(row == 1)
    def _():
        extra.start()
        for step in (PEN, TAIL, END):
            b_copy(step).start()

    def multiply(parts, first=0, count=ROWS, tm=512, columns=(0, COLS), fresh=False, out=acc):
        across = (columns[1] - columns[0]) // TN

        @pl.loop(0, (count // tm) * across)
        def _(t):
            rows = pl.ds(pl.multiple_of(first + (t // across) * tm, 64), tm)
            cols = pl.ds(pl.multiple_of(columns[0] + (t % across) * TN, TN), TN)
            lhs = jnp.concatenate([a4[s, rows, k] for s, k in parts], axis=1)
            rhs = jnp.concatenate([b4[s, k, cols] for s, k in parts], axis=0)
            part = jnp.dot(lhs, rhs, preferred_element_type=F32)
            out[rows, cols] = (part if fresh else acc[rows, cols] + part).astype(out.dtype)

    whole = pl.ds(0, Q)
    multiply([(0, whole)], fresh=True)

    for step in range(EARLY):
        b_copy(step).wait_recv()
        forward(step, pair).start()
        a_copy(step).wait_recv()
        forward(step, other).wait_recv()
        k = pl.ds(B_STEPS[step][0], B_STEPS[step][1])
        multiply([(1, k), (3, k)])
        slot, first, rows = A_STEPS[step]
        if slot == 2:
            multiply([(2, whole)], first, rows, tm=256)

    ends = pl.ds(B_STEPS[PEN][0], B_STEPS[PEN][1])
    alast[:, pl.ds(0, 128)] = a4[1, :, ends]
    alast[:, pl.ds(128, 128)] = a4[3, :, ends]

    @pl.when(row == 1)
    def _():
        relay_send.wait_recv()
        relay_end.start()
        extra.wait_recv()
        forward(END, other, more).start()

    done_rows = A_STEPS[LAST][1]
    b_copy(PEN).wait_recv()
    forward(PEN, pair).start()
    a_copy(PEN).wait_recv()
    multiply([(2, whole)], A_STEPS[PEN][1], A_STEPS[PEN][2], tm=128)
    forward(PEN, other).wait_recv()
    multiply([(1, ends), (3, ends)], 0, done_rows, tm=448, columns=(0, LEFT), out=left)
    multiply([(1, ends), (3, ends)], done_rows, ROWS - done_rows, tm=128, columns=(0, LEFT))

    def last_rows():
        multiply([(2, whole)], done_rows, ROWS - done_rows, tm=128, columns=(LEFT, COLS))
        multiply([(2, whole)], done_rows, ROWS - done_rows, tm=128, columns=(0, LEFT), out=left)

    @pl.when(row == 0)
    def _():
        a_copy(LAST, KEEP).wait_recv()
        relay_end.wait_recv()

    @pl.when(row == 1)
    def _():
        b_copy(TAIL).wait_recv()
        forward(TAIL, pair).start()
        b_copy(END).wait_recv()
        forward(END, pair).start()
        a_copy(LAST).wait_recv()

    last_rows()

    @pl.when(row == 0)
    def _():
        b_copy(TAIL).wait_recv()
        forward(TAIL, pair).start()

    forward(TAIL, other).wait_recv()

    @pl.when(row == 0)
    def _():
        forward(END, pair).wait_recv()
        forward(END, other).wait_recv()
        every = b4.at[:, pl.ds(0, Q - Q // 64)]
        pltpu.make_async_copy(every, every, main).wait()
        pltpu.make_async_copy(relay_out, relay_out, more).wait()

    @pl.when(row == 1)
    def _():
        pltpu.make_async_copy(b4, b4, main).wait()
        rest = alast.at[pl.ds(0, 768)]
        pltpu.make_async_copy(rest, rest, more).wait()


def finish_kernel(acc, left, alast, blast, c_ref, stage, done):
    pltpu.make_async_copy(left, c_ref.at[:, pl.ds(0, LEFT)], done).start()
    blk = 256
    right = pl.ds(LEFT, COLS - LEFT)
    for t in range(ROWS // blk):
        rows = pl.ds(t * blk, blk)
        tail = jnp.dot(alast[rows, :], blast[...], preferred_element_type=F32)
        stage[rows, :] = (acc[rows, right] + tail).astype(BF16)
        pltpu.make_async_copy(stage.at[rows], c_ref.at[rows, right], done).start()
    pltpu.make_async_copy(c_ref, c_ref, done).wait()


def solution(mesh):
    hbm = pl.BlockSpec(memory_space=pltpu.HBM)
    vmem = pl.BlockSpec(memory_space=pltpu.VMEM)
    dma = pltpu.SemaphoreType.DMA

    def local_product(a_blk, b_blk):
        a_blk = pltpu.with_memory_space_constraint(a_blk, pltpu.HBM)
        b_blk = pltpu.with_memory_space_constraint(b_blk, pltpu.HBM)
        partial = pl.pallas_call(
            exchange_kernel,
            out_shape=(
                pltpu.VMEM((ROWS, COLS), F32),
                pltpu.VMEM((ROWS, LEFT), BF16),
                pltpu.VMEM((ROWS, 256), BF16),
                pltpu.VMEM((256, COLS - LEFT), BF16),
            ),
            in_specs=[hbm, hbm],
            out_specs=(vmem,) * 4,
            scratch_shapes=[
                pltpu.VMEM((4, ROWS, Q), BF16),
                pltpu.VMEM((4, Q, COLS), BF16),
                pltpu.VMEM((64, Q), BF16),
                pltpu.VMEM((64, Q), BF16),
                pltpu.SemaphoreType.REGULAR((3,)),
                dma, dma((2,)), dma((LAST + 1,)), dma((2, END + 1)), dma, dma((2,)),
            ],
            compiler_params=pltpu.CompilerParams(
                collective_id=0, has_side_effects=True, vmem_limit_bytes=44 * 2**20),
            name="exchange",
        )(a_blk, b_blk)
        return pl.pallas_call(
            finish_kernel,
            out_shape=pltpu.HBM((ROWS, COLS), BF16),
            in_specs=[vmem] * 4,
            out_specs=hbm,
            scratch_shapes=[pltpu.VMEM((ROWS, COLS - LEFT), BF16), dma],
            compiler_params=pltpu.CompilerParams(vmem_limit_bytes=24 * 2**20),
            name="finish",
        )(*partial)

    spec = P(("row", "depth"), "col")
    return jax.shard_map(local_product, mesh=mesh, in_specs=(spec, spec), out_specs=spec, check_vma=False)
```

```python
import jax
import jax.numpy as jnp
from jax import lax
from jax.experimental import pallas as pl
from jax.experimental.pallas import tpu as pltpu
from jax.sharding import PartitionSpec as P

MESH = pl.DeviceIdType.MESH
BF16, F32 = jnp.bfloat16, jnp.float32

Q = 1024
ROWS, COLS = 1024, 2048

B_STEPS = [(0, 512, 0, COLS), (512, 256, 0, COLS), (768, 128, 0, COLS), (896, 128, 0, 1024), (896, 128, 1024, 768),
           (896, 128, 1792, 256)]
A_STEPS = [(3, 0, ROWS), (2, 0, 512), (2, 512, 256), (2, 768, 128), (2, 896, 128)]
EARLY = 3
PEN, TAIL, END = 3, 4, 5
LAST = 4
LEFT = 1024
KEEP = 64
TN = 1024


def exchange_kernel(a_ref, b_ref, acc, left, alast, blast, a4, b4, relay_out, relay_in,
                    ready, loaded, sent, last, yr, direct, fin, relayed):
    dep, col, row = lax.axis_index("depth"), lax.axis_index("col"), lax.axis_index("row")
    x_nbr, y_nbr, sib = (dep, 1 - col, row), (1 - dep, col, row), (dep, col, 1 - row)
    pair = (row + col) % 2
    other = 1 - pair
    near = pl.multiple_of(dep * Q, Q)
    far = pl.multiple_of((1 - dep) * Q, Q)
    main, more = sent.at[0], sent.at[1]

    def remote(src, dst, send_sem, recv_sem, dev):
        return pltpu.make_async_remote_copy(src, dst, send_sem, recv_sem, device_id=dev, device_id_type=MESH)

    barrier = pltpu.get_barrier_semaphore()

    def tell(semaphore, dev):
        pl.semaphore_signal(semaphore, inc=1, device_id=dev, device_id_type=MESH)

    pl.when(col == 0)(lambda: tell(barrier, x_nbr))
    pl.when(dep == 0)(lambda: tell(barrier, y_nbr))
    pl.when(row == 1)(lambda: tell(barrier, sib))
    heard = col + dep + (1 - row)
    pl.when(heard > 0)(lambda: pl.semaphore_wait(barrier, heard))
    pl.when(col == 1)(lambda: tell(ready.at[0], x_nbr))
    pl.when(dep == 1)(lambda: tell(ready.at[1], y_nbr))
    pl.when(row == 0)(lambda: tell(ready.at[2], sib))

    def a_copy(step, keep=None):
        slot, first, rows = A_STEPS[step]
        rows = pl.ds(first, keep or rows)
        src = a_ref.at[rows, pl.ds(near if slot == 2 else far, Q)]
        return remote(src, a4.at[slot, rows], main, last if step == LAST else yr.at[other, step], x_nbr)

    def b_place(step, which):
        r, rows, c, cols = B_STEPS[step]
        if step >= TAIL:
            return blast.at[pl.ds(pl.multiple_of(which * rows, rows), rows), pl.ds(c - LEFT, cols)]
        return b4.at[2 * which + 1, pl.ds(r, rows), pl.ds(c, cols)]

    def b_copy(step):
        r, rows, c, cols = B_STEPS[step]
        return remote(b_ref.at[pl.ds(r, rows), pl.ds(c, cols)], b_place(step, pair), main,
                      direct.at[step - TAIL] if step >= TAIL else yr.at[pair, step], y_nbr)

    def forward(step, which, sem=main):
        return remote(b_place(step, which), b_place(step, which), sem, fin if step >= TAIL else yr.at[which, step], sib)

    end_rows, end_cols = pl.ds(B_STEPS[END][0], B_STEPS[END][1]), pl.ds(B_STEPS[END][2], B_STEPS[END][3])
    extra = remote(b4.at[2 * other, end_rows, end_cols], b_place(END, other), more, direct.at[2], y_nbr)
    relay_rows = pl.ds(A_STEPS[LAST][1] + KEEP, A_STEPS[LAST][2] - KEEP)
    relay_give = remote(a_ref.at[relay_rows, pl.ds(near, Q)], relay_out, more, relayed, sib)
    relay_send = remote(relay_out, relay_in, more, direct.at[2], x_nbr)
    relay_end = remote(relay_in, a4.at[2, relay_rows], more, last, sib)

    give = remote(b_ref, b4.at[2 * pair], main, loaded, sib)

    def all_of(semaphore, ref):
        pltpu.make_async_copy(ref, ref, semaphore).wait()

    def pieces(*sizes):
        return b4.at[0, pl.ds(0, sum(sizes) // COLS)]

    def size(step):
        return B_STEPS[step][1] * B_STEPS[step][3]


    def send_b():
        for step in range(EARLY):
            b_copy(step).start()

    pl.when(dep == 1)(send_b)
    pl.when(col == 0)(lambda: pl.semaphore_wait(ready.at[0], 1))
    for step in range(EARLY):
        a_copy(step).start()

    @pl.when(dep == 0)
    def _():
        pl.semaphore_wait(ready.at[1], 1)
        send_b()

    pl.when(row == 1)(lambda: pl.semaphore_wait(ready.at[2], 1))
    pltpu.make_async_copy(a_ref.at[:, pl.ds(near, Q)], a4.at[0], loaded).start()
    pltpu.make_async_copy(a_ref.at[:, pl.ds(far, Q)], a4.at[1], loaded).start()
    pltpu.make_async_copy(b_ref, b4.at[2 * pair], loaded).start()

    @pl.when(row == 0)
    def _():
        relay_give.start()
        a_copy(PEN).start()
        a_copy(LAST, KEEP).start()
        b_copy(PEN).start()
        b_copy(TAIL).start()

    give.start()

    @pl.when(row == 1)
    def _():
        relay_give.wait_recv()
        relay_send.start()
        a_copy(PEN).start()
        a_copy(LAST).start()

    all_of(loaded, b4.at[pl.ds(0, 3)])

    @pl.when(row == 1)
    def _():
        extra.start()
        for step in (PEN, TAIL, END):
            b_copy(step).start()

    def multiply(parts, first=0, count=ROWS, tm=512, columns=(0, COLS), fresh=False, out=acc):
        across = (columns[1] - columns[0]) // TN

        @pl.loop(0, (count // tm) * across)
        def _(t):
            rows = pl.ds(pl.multiple_of(first + (t // across) * tm, 64), tm)
            cols = pl.ds(pl.multiple_of(columns[0] + (t % across) * TN, TN), TN)
            lhs = jnp.concatenate([a4[s, rows, k] for s, k in parts], axis=1)
            rhs = jnp.concatenate([b4[s, k, cols] for s, k in parts], axis=0)
            part = jnp.dot(lhs, rhs, preferred_element_type=F32)
            out[rows, cols] = (part if fresh else acc[rows, cols] + part).astype(out.dtype)

    whole = pl.ds(0, Q)
    multiply([(0, whole)], fresh=True)

    for step in range(EARLY):
        all_of(yr.at[pair, step], pieces(size(step), A_STEPS[step][2] * Q))
        forward(step, pair).start()
        forward(step, other).wait_recv()
        k = pl.ds(B_STEPS[step][0], B_STEPS[step][1])
        multiply([(1, k), (3, k)])
        slot, first, rows = A_STEPS[step]
        if slot == 2:
            multiply([(2, whole)], first, rows, tm=256)

    ends = pl.ds(B_STEPS[PEN][0], B_STEPS[PEN][1])
    alast[:, pl.ds(0, 128)] = a4[1, :, ends]
    alast[:, pl.ds(128, 128)] = a4[3, :, ends]

    @pl.when(row == 1)
    def _():
        all_of(direct.at[2], pieces(size(END), (ROWS - A_STEPS[LAST][1] - KEEP) * Q))
        relay_end.start()
        forward(END, other, more).start()

    done_rows = A_STEPS[LAST][1]
    all_of(yr.at[pair, PEN], pieces(size(PEN), A_STEPS[PEN][2] * Q))
    forward(PEN, pair).start()
    multiply([(2, whole)], A_STEPS[PEN][1], A_STEPS[PEN][2], tm=128)
    forward(PEN, other).wait_recv()
    multiply([(1, ends), (3, ends)], 0, done_rows, tm=448, columns=(0, LEFT), out=left)
    multiply([(1, ends), (3, ends)], done_rows, ROWS - done_rows, tm=128, columns=(0, LEFT))

    def last_rows():
        multiply([(2, whole)], done_rows, ROWS - done_rows, tm=128, columns=(LEFT, COLS))
        multiply([(2, whole)], done_rows, ROWS - done_rows, tm=128, columns=(0, LEFT), out=left)

    @pl.when(row == 1)
    def _():
        b_copy(TAIL).wait_recv()
        forward(TAIL, pair).start()
        b_copy(END).wait_recv()
        forward(END, pair).start()

    a_copy(LAST).wait_recv()
    last_rows()

    @pl.when(row == 0)
    def _():
        b_copy(TAIL).wait_recv()
        forward(TAIL, pair).start()

    @pl.when(row == 0)
    def _():
        all_of(fin, pieces(size(TAIL), size(END), size(END)))
        all_of(main, b4.at[:, pl.ds(0, Q - Q // 64)])
        all_of(more, relay_out)

    @pl.when(row == 1)
    def _():
        all_of(fin, pieces(size(TAIL)))
        all_of(main, b4)
        all_of(more, alast.at[pl.ds(0, 768)])


def finish_kernel(acc, left, alast, blast, c_ref, stage, done):
    pltpu.make_async_copy(left, c_ref.at[:, pl.ds(0, LEFT)], done).start()
    blk = 128
    right = pl.ds(LEFT, COLS - LEFT)
    for t in range(ROWS // blk):
        rows = pl.ds(t * blk, blk)
        tail = jnp.dot(alast[rows, :], blast[...], preferred_element_type=F32)
        stage[rows, :] = (acc[rows, right] + tail).astype(BF16)
        pltpu.make_async_copy(stage.at[rows], c_ref.at[rows, right], done).start()
    pltpu.make_async_copy(c_ref, c_ref, done).wait()


def solution(mesh):
    hbm = pl.BlockSpec(memory_space=pltpu.HBM)
    vmem = pl.BlockSpec(memory_space=pltpu.VMEM)
    dma = pltpu.SemaphoreType.DMA

    def local_product(a_blk, b_blk):
        a_blk = pltpu.with_memory_space_constraint(a_blk, pltpu.HBM)
        b_blk = pltpu.with_memory_space_constraint(b_blk, pltpu.HBM)
        partial = pl.pallas_call(
            exchange_kernel,
            out_shape=(
                pltpu.VMEM((ROWS, COLS), F32),
                pltpu.VMEM((ROWS, LEFT), BF16),
                pltpu.VMEM((ROWS, 256), BF16),
                pltpu.VMEM((256, COLS - LEFT), BF16),
            ),
            in_specs=[hbm, hbm],
            out_specs=(vmem,) * 4,
            scratch_shapes=[
                pltpu.VMEM((4, ROWS, Q), BF16),
                pltpu.VMEM((4, Q, COLS), BF16),
                pltpu.VMEM((64, Q), BF16),
                pltpu.VMEM((64, Q), BF16),
                pltpu.SemaphoreType.REGULAR((3,)),
                dma, dma((2,)), dma, dma((2, TAIL)), dma((3,)), dma, dma,
            ],
            compiler_params=pltpu.CompilerParams(
                collective_id=0, has_side_effects=True, vmem_limit_bytes=44 * 2**20),
            name="exchange",
        )(a_blk, b_blk)
        return pl.pallas_call(
            finish_kernel,
            out_shape=pltpu.HBM((ROWS, COLS), BF16),
            in_specs=[vmem] * 4,
            out_specs=hbm,
            scratch_shapes=[pltpu.VMEM((ROWS, COLS - LEFT), BF16), dma],
            compiler_params=pltpu.CompilerParams(vmem_limit_bytes=24 * 2**20),
            name="finish",
        )(*partial)

    spec = P(("row", "depth"), "col")
    return jax.shard_map(local_product, mesh=mesh, in_specs=(spec, spec), out_specs=spec, check_vma=False)
```
